16 devices in a mesh: dp: 2 (over y, z), tp: 8 (over x, core).
Axes of the slice: x: 4, y: 2, z: 1, core: 2. Of those that a mesh axis runs over, the one named last changes fastest.
The devices are a block of a 4x4x8 slice.
Arguments:
- x: bfloat16 [4096, 2048], P('dp'), parts along dimension 0
- dy: bfloat16 [4096, 2048], P('dp'), parts along dimension 0
- gate: bfloat16 [4096, 6144], P('dp', 'tp'), parts along dimension 0
- up: bfloat16 [4096, 6144], P('dp', 'tp'), parts along dimension 0
- w_gate: bfloat16 [2048, 6144], P(None, 'tp')
- w_up: bfloat16 [2048, 6144], P(None, 'tp')
- w_down: bfloat16 [6144, 2048], P('tp')
Outputs:
- output 1: bfloat16 [4096, 2048], P('dp'), parts along dimension 0
- output 2: bfloat16 [4096, 6144], P('dp', 'tp'), parts along dimension 0
- output 3: bfloat16 [4096, 6144], P('dp', 'tp'), parts along dimension 0
- output 4: bfloat16 [12288, 2048], P(('dp', 'tp')), parts along dimension 0
There are 2 independent parts. The reference program is written for one: setup_inputs(seed, part) draws one part's arguments, and reference() takes and returns one part's arrays. A program takes and returns all parts, laid end to end along the dimension named above; an argument that names none is the same for every part.
All inputs are finite; a program needn't handle non-finite values.
Results may differ from the reference program's by a relative error of at most 0.012.
Values are sent between devices in bfloat16 or wider.
A program may use at most 768 MiB of HBM per device.

```python
import jax
import jax.numpy as jnp

ROWS = 2048
D = 2048
FF = 6144


def act(gate, up):
    return jax.nn.silu(gate) * up


def setup_inputs(seed: int = 0, part: int = 0) -> dict:
    kx, ky, ka, kb, kg, ku, kd = jax.random.split(jax.random.key(seed), 7)
    kx, ky, ka, kb = (jax.random.fold_in(k, part) for k in (kx, ky, ka, kb))
    drawn = {
        "x": jax.random.normal(kx, (ROWS, D), jnp.float32),
        "dy": jax.random.normal(ky, (ROWS, D), jnp.float32),
        "gate": jax.random.normal(ka, (ROWS, FF), jnp.float32),
        "up": jax.random.normal(kb, (ROWS, FF), jnp.float32),
        "w_gate": jax.random.normal(kg, (D, FF), jnp.float32) * D**-0.5,
        "w_up": jax.random.normal(ku, (D, FF), jnp.float32) * D**-0.5,
        "w_down": jax.random.normal(kd, (FF, D), jnp.float32) * FF**-0.5,
    }
    return {k: v.astype(jnp.bfloat16) for k, v in drawn.items()}


def reference(x, dy, gate, up, w_gate, w_up, w_down):
    hidden, back = jax.vjp(act, gate.astype(jnp.float32), up.astype(jnp.float32))
    d_hidden = jnp.dot(dy, w_down.T, preferred_element_type=jnp.float32)
    d_gate, d_up = (g.astype(jnp.bfloat16) for g in back(d_hidden))
    dx = jnp.dot(d_gate, w_gate.T, preferred_element_type=jnp.float32) + jnp.dot(d_up, w_up.T, preferred_element_type=jnp.float32)
    dw_gate = jnp.dot(x.T, d_gate, preferred_element_type=jnp.float32)
    dw_up = jnp.dot(x.T, d_up, preferred_element_type=jnp.float32)
    dw_down = jnp.dot(hidden.astype(jnp.bfloat16).T, dy, preferred_element_type=jnp.float32)
    return tuple(g.astype(jnp.bfloat16) for g in (dx, dw_gate, dw_up, dw_down))
```

```python
import functools

import jax
import jax.numpy as jnp
from jax import lax
from jax.experimental import pallas as pl
from jax.experimental.pallas import tpu as pltpu
from jax.sharding import PartitionSpec as P

BF16, F32 = jnp.bfloat16, jnp.float32
ANY = pl.BlockSpec(memory_space=pl.ANY)
VMEM = pl.BlockSpec(memory_space=pltpu.VMEM)
PIECES = 4
TILE = 256


def dot(a, b, a_dim, b_dim):
    return lax.dot_general(a, b, (((a_dim,), (b_dim,)), ((), ())), preferred_element_type=F32)


def work(
    chips, x, dy, gate, up, w_gate, w_up, w_down, dx, wg, wu, wd,
    own, got, ring, mate, dys, dgs, dus, hid, gs, us, xs,
    load, wload, xload, pair_s, pair_r, rs_s, rs_r, ag_s, ag_r, fin_s, fin_r,
):
    rows, width = dx.shape
    hidden = wd.shape[0]
    block = rows // (4 * chips)
    part = width // PIECES
    t = lax.axis_index("tp")
    k, c = t // 2, t % 2
    right = {"tp": (k + 1) % chips * 2 + c}
    left = {"tp": (k + chips - 1) % chips * 2 + c}
    partner = {"tp": k * 2 + 1 - c}
    ways = (right, left)

    def origin(d, hops):
        return (k + chips - hops) % chips if d == 0 else (k + hops) % chips

    def row(chunk, d, core):
        return pl.multiple_of((chunk * 4 + d * 2 + core) * block, block)

    def segments(s):
        todo = [(k + 2 * chips - 1 - s) % chips, (k + 1 + s) % chips]
        return [row(todo[d], d, core) for core in (c, 1 - c) for d in (0, 1)]

    def load_dy(s):
        for i, r in enumerate(segments(s)):
            pltpu.make_async_copy(
                dy.at[pl.ds(r, block)], dys.at[pl.ds((4 * s + i) * block, block)], load.at[0, s]
            ).start()

    def load_act(s):
        for i, r in enumerate(segments(s)):
            for n, (src, dst) in enumerate(((gate, gs), (up, us))):
                pltpu.make_async_copy(
                    src.at[pl.ds(r, block)], dst.at[s % 2, pl.ds(i * block, block)], load.at[1 + n, s]
                ).start()

    def load_x(b):
        for s in range(chips):
            for i, r in enumerate(segments(s)):
                pltpu.make_async_copy(
                    x.at[pl.ds(r, block), pl.ds(b * part, part)],
                    xs.at[b % 2, pl.ds((4 * s + i) * block, block)],
                    xload.at[b],
                ).start()

    def weights(src, dst, n, sem):
        size = src.shape[0] // n
        return [
            pltpu.make_async_copy(src.at[pl.ds(i * size, size)], dst.at[pl.ds(i * size, size)], wload.at[sem, i])
            for i in range(n)
        ]

    wd_loads = weights(w_down, wd, hidden // TILE, 0)
    wg_loads = weights(w_gate, wg, PIECES, 1)
    wu_loads = weights(w_up, wu, PIECES, 2)
    load_dy(0)
    for copy in wd_loads:
        copy.start()
    load_act(0)
    for a, b in zip(wg_loads, wu_loads):
        a.start()
        b.start()
    for s in range(1, chips):
        load_dy(s)
    load_act(1)
    load_x(0)
    load_x(1)

    barrier = pltpu.get_barrier_semaphore()
    for other in (right, left, partner):
        pl.semaphore_signal(barrier, inc=1, device_id=other)
    pl.semaphore_wait(barrier, 3)

    def remote(src, dst, send, recv, to):
        return pltpu.make_async_remote_copy(src_ref=src, dst_ref=dst, send_sem=send, recv_sem=recv, device_id=to)

    def pair(s, q):
        at = (pl.ds(0, 2 * block), pl.ds(q * part, part))
        return remote(mate.at[s % 2, *at], got.at[s, *at], pair_s.at[s, q], pair_r.at[s, q], partner)

    def reduce(d, s, q):
        cols = pl.ds(q * part, part)
        return remote(
            got.at[s, pl.ds(d * block, block), cols], ring.at[d, s, :, cols], rs_s.at[d, s, q], rs_r.at[d, s, q], ways[d]
        )

    def gather(d, hops, q):
        at = dx.at[pl.ds(row(origin(d, hops), d, c), block), pl.ds(q * part, part)]
        return remote(at, at, ag_s.at[d, hops, q], ag_r.at[d, hops, q], ways[d])

    def share(d, hops, q):
        at = dx.at[pl.ds(row(origin(d, hops), d, c), block), pl.ds(q * part, part)]
        return remote(at, at, fin_s.at[d, hops, q], fin_r.at[d, hops, q], partner)

    def pass_on(s, q):
        cols = pl.ds(q * part, part)
        pair(s, q).wait_recv()
        for d in (0, 1):
            band = pl.ds(d * block, block)
            total = own[s, band, cols] + got[s, band, cols].astype(F32)
            if s > 0:
                reduce(d, s - 1, q).wait_recv()
                total = total + ring[d, s - 1, :, cols].astype(F32)
            if s < chips - 1:
                got[s, band, cols] = total.astype(BF16)
            else:
                dx[pl.ds(row(k, d, c), block), cols] = total.astype(BF16)
        for d in (0, 1):
            if s < chips - 1:
                reduce(d, s, q).start()
            else:
                gather(d, 0, q).start()
        if s == chips - 1:
            for d in (0, 1):
                share(d, 0, q).start()

    def forward(hops, q):
        for d in (0, 1):
            gather(d, hops - 1, q).wait_recv()
            if hops < chips - 1:
                gather(d, hops, q).start()
            share(d, hops, q).start()

    for s in range(chips):
        here = pl.ds(4 * s * block, 4 * block)
        pltpu.make_async_copy(dy.at[pl.ds(0, 4 * block)], dys.at[here], load.at[0, s]).wait()

        def act_back(i, s=s, here=here):
            cols = pl.ds(pl.multiple_of(i * TILE, TILE), TILE)
            dh = dot(dys[here], wd[cols, :], 1, 1)
            g = gs[s % 2, :, cols].astype(F32)
            u = us[s % 2, :, cols].astype(F32)
            sig = lax.logistic(g)
            silu = g * sig
            ct = dh * u
            hid[here, cols] = (silu * u).astype(BF16)
            dus[here, cols] = (dh * silu).astype(BF16)
            dgs[here, cols] = (ct * sig + (ct * g) * (sig * (1.0 - sig))).astype(BF16)

        def wait_act(s=s):
            pltpu.make_async_copy(gate.at[pl.ds(0, 4 * block)], gs.at[s % 2], load.at[1, s]).wait()
            pltpu.make_async_copy(up.at[pl.ds(0, 4 * block)], us.at[s % 2], load.at[2, s]).wait()

        if s == 0:
            for i in range(hidden // TILE):
                wd_loads[i].wait()
                if i == 0:
                    wait_act()
                act_back(i)
        else:
            wait_act()
            pl.loop(0, hidden // TILE)(act_back)
        if s + 2 < chips:
            load_act(s + 2)

        for q in range(PIECES):
            if s == 0:
                wg_loads[q].wait()
                wu_loads[q].wait()
            if s >= 2:
                pair(s - 2, q).wait_send()

            def term(i, s=s, q=q, here=here):
                cols = pl.ds(pl.multiple_of(q * part + i * TILE, TILE), TILE)
                v = dot(dgs[here, :], wg[cols, :], 1, 1) + dot(dus[here, :], wu[cols, :], 1, 1)
                own[s, :, cols] = v[: 2 * block]
                mate[s % 2, :, cols] = v[2 * block :].astype(BF16)

            pl.loop(0, part // TILE)(term)
            pair(s, q).start()
            if q > 0:
                pass_on(s, q - 1)
        pass_on(s, PIECES - 1)

    events = [(hops, q) for hops in range(1, chips) for q in range(PIECES)]

    def columns_of(i):
        return pl.ds(pl.multiple_of(i * TILE, TILE), TILE)

    for b in range(PIECES):
        band = pl.ds(b * part, part)
        pltpu.make_async_copy(x.at[:, band], xs.at[b % 2], xload.at[b]).wait()

        @pl.loop(0, hidden // TILE)
        def _(i, b=b, band=band):
            wg[band, columns_of(i)] = dot(xs[b % 2], dgs[:, columns_of(i)], 0, 0).astype(BF16)

        if b > 0:
            forward(*events.pop(0))

        @pl.loop(0, hidden // TILE)
        def _(i, b=b, band=band):
            wu[band, columns_of(i)] = dot(xs[b % 2], dus[:, columns_of(i)], 0, 0).astype(BF16)

        if b + 2 < PIECES:
            load_x(b + 2)
        forward(*events.pop(0))

        @pl.loop(0, part // TILE)
        def _(i, b=b):
            cols = pl.ds(pl.multiple_of(b * part + i * TILE, TILE), TILE)
            wd[:, cols] = dot(hid[...], dys[:, cols], 0, 0).astype(BF16)

    while events:
        forward(*events.pop(0))

    for q in range(PIECES):
        for s in range(max(chips - 2, 0), chips):
            pair(s, q).wait_send()
        for d in (0, 1):
            for s in range(chips - 1):
                reduce(d, s, q).wait_send()
                gather(d, s, q).wait_send()
            for s in range(chips):
                share(d, s, q).wait_send()
                share(d, s, q).wait_recv()


def store(*refs):
    n = (len(refs) - 1) // 2
    sems = refs[-1]
    for i, (src, dst) in enumerate(zip(refs[:n], refs[n:-1])):
        size = src.shape[0] // PIECES
        for p in range(PIECES):
            at = pl.ds(p * size, size)
            pltpu.make_async_copy(src.at[at], dst.at[at], sems.at[i]).start()
    for i, (src, dst) in enumerate(zip(refs[:n], refs[n:-1])):
        pltpu.make_async_copy(src, dst, sems.at[i]).wait()


def solution(mesh):
    chips = mesh.shape["tp"] // 2

    def step(x, dy, gate, up, w_gate, w_up, w_down):
        rows, width = x.shape
        hidden = gate.shape[1]
        block = rows // (4 * chips)
        shapes = ((rows, width), w_gate.shape, w_up.shape, w_down.shape)
        dma = pltpu.SemaphoreType.DMA
        outs = pl.pallas_call(
            functools.partial(work, chips),
            name="work",
            out_shape=[pltpu.VMEM(s, BF16) for s in shapes],
            in_specs=[ANY] * 7,
            out_specs=[VMEM] * 4,
            scratch_shapes=[
                pltpu.VMEM((chips, 2 * block, width), F32),
                pltpu.VMEM((chips, 2 * block, width), BF16),
                pltpu.VMEM((2, chips - 1, block, width), BF16),
                pltpu.VMEM((2, 2 * block, width), BF16),
                pltpu.VMEM((rows, width), BF16),
                pltpu.VMEM((rows, hidden), BF16),
                pltpu.VMEM((rows, hidden), BF16),
                pltpu.VMEM((rows, hidden), BF16),
                pltpu.VMEM((2, 4 * block, hidden), BF16),
                pltpu.VMEM((2, 4 * block, hidden), BF16),
                pltpu.VMEM((2, rows, width // PIECES), BF16),
                dma((3, chips)),
                dma((3, PIECES)),
                dma((PIECES,)),
                dma((chips, PIECES)),
                dma((chips, PIECES)),
                dma((2, chips - 1, PIECES)),
                dma((2, chips - 1, PIECES)),
                dma((2, chips - 1, PIECES)),
                dma((2, chips - 1, PIECES)),
                dma((2, chips, PIECES)),
                dma((2, chips, PIECES)),
            ],
            compiler_params=pltpu.CompilerParams(
                collective_id=0, has_side_effects=True, vmem_limit_bytes=46 * 2**20
            ),
        )(x, dy, gate, up, w_gate, w_up, w_down)
        return pl.pallas_call(
            store,
            name="store",
            out_shape=[jax.ShapeDtypeStruct(s, BF16) for s in shapes],
            in_specs=[VMEM] * 4,
            out_specs=[ANY] * 4,
            scratch_shapes=[dma((4,))],
            compiler_params=pltpu.CompilerParams(vmem_limit_bytes=2**20),
        )(*(pltpu.with_memory_space_constraint(o, pltpu.VMEM) for o in outs))

    tokens, columns, down = P("dp", None), P(None, "tp"), P("tp", None)
    return jax.shard_map(
        step,
        mesh=mesh,
        in_specs=(tokens, tokens, P("dp", "tp"), P("dp", "tp"), columns, columns, down),
        out_specs=(tokens, P("dp", "tp"), P("dp", "tp"), P(("dp", "tp"), None)),
        check_vma=False,
    )
```

```python
import functools

import jax
import jax.numpy as jnp
from jax import lax
from jax.experimental import pallas as pl
from jax.experimental.pallas import tpu as pltpu
from jax.sharding import PartitionSpec as P

BF16, F32 = jnp.bfloat16, jnp.float32
ANY = pl.BlockSpec(memory_space=pl.ANY)
VMEM = pl.BlockSpec(memory_space=pltpu.VMEM)
PIECES = 4
TILE = 256


def dot(a, b, a_dim, b_dim):
    return lax.dot_general(a, b, (((a_dim,), (b_dim,)), ((), ())), preferred_element_type=F32)


def work(
    chips, x, dy, gate, up, w_gate, w_up, w_down, dx, wg, wu, wd,
    own, got, ring, mate, dys, dgu, hid, gs, us, wgu,
    load, wload, xload, pair_s, pair_r, rs_s, rs_r, ag_s, ag_r, fin_s, fin_r,
):
    rows, width = dx.shape
    hidden = wd.shape[0]
    block = rows // (4 * chips)
    part = width // PIECES
    t = lax.axis_index("tp")
    k, c = t // 2, t % 2
    right = {"tp": (k + 1) % chips * 2 + c}
    left = {"tp": (k + chips - 1) % chips * 2 + c}
    partner = {"tp": k * 2 + 1 - c}
    ways = (right, left)

    def origin(d, hops):
        return (k + chips - hops) % chips if d == 0 else (k + hops) % chips

    def row(chunk, d, core):
        return pl.multiple_of((chunk * 4 + d * 2 + core) * block, block)

    units = [(0, 0), (0, 1)] + [(s, 0) for s in range(1, chips)]

    def high(s):
        return block // 2 if s == 0 else block

    def halves(s):
        return (0, 1) if s == 0 else (0,)

    def number(s, h):
        return units.index((s, h))

    def begin(s, h):
        return 4 * (s * block + h * high(s))

    def segments(s, h):
        todo = [(k + 2 * chips - 1 - s) % chips, (k + 1 + s) % chips]
        return [row(todo[d], d, core) + h * high(s) for core in (c, 1 - c) for d in (0, 1)]

    def load_dy(s, h):
        n = high(s)
        for i, r in enumerate(segments(s, h)):
            pltpu.make_async_copy(
                dy.at[pl.ds(r, n)], dys.at[pl.ds(begin(s, h) + i * n, n)], load.at[0, number(s, h)]
            ).start()

    def load_act(s, h):
        n = high(s)
        for i, r in enumerate(segments(s, h)):
            for m, (src, dst) in enumerate(((gate, gs), (up, us))):
                pltpu.make_async_copy(
                    src.at[pl.ds(r, n)],
                    dst.at[s % 2, pl.ds((h * 4 + i) * n, n)],
                    load.at[1 + m, number(s, h)],
                ).start()

    def load_x(b):
        for s, h in units:
            n = high(s)
            for i, r in enumerate(segments(s, h)):
                pltpu.make_async_copy(
                    x.at[pl.ds(r, n), pl.ds(b * part, part)],
                    wgu.at[pl.ds(begin(s, h) + i * n, n), pl.ds(b % 2 * part, part)],
                    xload.at[b],
                ).start()

    def weights(q):
        band = pl.ds(q * part, part)
        return [
            pltpu.make_async_copy(src.at[band], wgu.at[band, pl.ds(m * hidden, hidden)], wload.at[m, q])
            for m, src in enumerate((w_gate, w_up))
        ]

    def start(copies):
        for copy in copies:
            copy.start()

    def weights_down(i):
        n = TILE // PIECES
        for j in range(PIECES):
            band = pl.ds(i * TILE + j * n, n)
            pltpu.make_async_copy(w_down.at[band], wd.at[band], wload.at[2, i]).start()

    def wait_weights_down(i):
        band = pl.ds(i * TILE, TILE)
        pltpu.make_async_copy(w_down.at[band], wd.at[band], wload.at[2, i]).wait()

    load_act(0, 0)
    load_dy(0, 0)
    for i in range(hidden // TILE):
        weights_down(i)
    start(weights(0))

    barrier = pltpu.get_barrier_semaphore()
    for other in (right, left, partner):
        pl.semaphore_signal(barrier, inc=1, device_id=other)

    def remote(src, dst, send, recv, to):
        return pltpu.make_async_remote_copy(src_ref=src, dst_ref=dst, send_sem=send, recv_sem=recv, device_id=to)

    def pair(s, h, q):
        at = (pl.ds(h * 2 * high(s), 2 * high(s)), pl.ds(q * part, part))
        u = number(s, h)
        return remote(mate.at[s % 2, *at], got.at[s, *at], pair_s.at[u, q], pair_r.at[u, q], partner)

    def reduce(d, s, h, q):
        cols = pl.ds(q * part, part)
        n, u = high(s), number(s, h)
        return remote(
            got.at[s, pl.ds((h * 2 + d) * n, n), cols],
            ring.at[d, s, pl.ds(h * n, n), cols],
            rs_s.at[d, u, q],
            rs_r.at[d, u, q],
            ways[d],
        )

    def gather(d, hops, q):
        at = dx.at[pl.ds(row(origin(d, hops), d, c), block), pl.ds(q * part, part)]
        return remote(at, at, ag_s.at[d, hops, q], ag_r.at[d, hops, q], ways[d])

    def share(d, hops, q):
        at = dx.at[pl.ds(row(origin(d, hops), d, c), block), pl.ds(q * part, part)]
        return remote(at, at, fin_s.at[d, hops, q], fin_r.at[d, hops, q], partner)

    def pass_on(s, h, q):
        cols = pl.ds(q * part, part)
        n = high(s)
        pair(s, h, q).wait_recv()
        for d in (0, 1):
            band = pl.ds((h * 2 + d) * n, n)
            total = own[s, band, cols] + got[s, band, cols].astype(F32)
            if s > 0:
                for before in halves(s - 1):
                    reduce(d, s - 1, before, q).wait_recv()
                total = total + ring[d, s - 1, :, cols].astype(F32)
            if s < chips - 1:
                got[s, band, cols] = total.astype(BF16)
            else:
                dx[pl.ds(row(k, d, c), block), cols] = total.astype(BF16)
        for d in (0, 1):
            if s < chips - 1:
                reduce(d, s, h, q).start()
            else:
                gather(d, 0, q).start()
        if s == chips - 1:
            for d in (0, 1):
                share(d, 0, q).start()

    def forward(hops, q):
        for d in (0, 1):
            gather(d, hops - 1, q).wait_recv()
            if hops < chips - 1:
                gather(d, hops, q).start()
            share(d, hops, q).start()

    waiting = []
    for s, h in units:
        n = high(s)
        here = pl.ds(begin(s, h), 4 * n)
        there = pl.ds(h * 4 * n, 4 * n)
        u = number(s, h)

        def gates(i, s=s, here=here, there=there):
            cols = pl.ds(pl.multiple_of(i * TILE, TILE), TILE)
            g = gs[s % 2, there, cols].astype(F32)
            v = us[s % 2, there, cols].astype(F32)
            sig = lax.logistic(g)
            silu = g * sig
            hid[here, cols] = (silu * v).astype(BF16)
            return silu, sig + g * (sig * (1.0 - sig)), v

        def back(i, silu, slope, v, here=here):
            cols = pl.ds(pl.multiple_of(i * TILE, TILE), TILE)
            up_cols = pl.ds(pl.multiple_of(hidden + i * TILE, TILE), TILE)
            dh = dot(dys[here], wd[cols, :], 1, 1)
            dgu[here, cols] = (dh * v * slope).astype(BF16)
            dgu[here, up_cols] = (dh * silu).astype(BF16)

        for m, (src, dst) in enumerate(((gate, gs), (up, us))):
            pltpu.make_async_copy(src.at[pl.ds(0, 4 * n)], dst.at[s % 2, there], load.at[1 + m, u]).wait()
        if u == 0:
            for i in range(hidden // TILE):
                silu, slope, _ = gates(i)
                own[chips - 1, pl.ds(0, 4 * n), pl.ds(i * TILE, TILE)] = silu
                own[chips - 1, pl.ds(0, 4 * n), pl.ds(hidden + i * TILE, TILE)] = slope
            pltpu.make_async_copy(dy.at[pl.ds(0, 4 * n)], dys.at[here], load.at[0, u]).wait()
            for i in range(hidden // TILE):
                wait_weights_down(i)
                if i > 0:
                    start(weights(i))
                silu = own[chips - 1, pl.ds(0, 4 * n), pl.ds(i * TILE, TILE)]
                slope = own[chips - 1, pl.ds(0, 4 * n), pl.ds(hidden + i * TILE, TILE)]
                back(i, silu, slope, us[0, there, pl.ds(i * TILE, TILE)].astype(F32))
            for q in range(hidden // TILE, PIECES):
                start(weights(q))
        else:
            pltpu.make_async_copy(dy.at[pl.ds(0, 4 * n)], dys.at[here], load.at[0, u]).wait()
            pl.loop(0, hidden // TILE)(lambda i: back(i, *gates(i)))
        if u + 1 < len(units):
            load_dy(*units[u + 1])
            load_act(*units[u + 1])

        for q in range(PIECES):
            if u == 0:
                for copy in weights(q):
                    copy.wait()
            if s >= 2:
                for before in halves(s - 2):
                    pair(s - 2, before, q).wait_send()
            cols = pl.ds(q * part, part)
            v = dot(dgu[here, :], wgu[cols, :], 1, 1)
            mate[s % 2, pl.ds(h * 2 * n, 2 * n), cols] = v[2 * n :].astype(BF16)
            if u == 0 and q == 0:
                pl.semaphore_wait(barrier, 3)
            pair(s, h, q).start()
            own[s, pl.ds(h * 2 * n, 2 * n), cols] = v[: 2 * n]
            waiting.append((s, h, q))
            while len(waiting) > (2 if s == 0 else 1):
                pass_on(*waiting.pop(0))
        if (s, h) == units[-1]:
            load_x(0)
            load_x(1)
    while waiting:
        pass_on(*waiting.pop(0))

    events = [(hops, q) for hops in range(1, chips) for q in range(PIECES)]

    for b in range(PIECES):
        band = pl.ds(b * part, part)
        slot = pl.ds(b % 2 * part, part)

        @pl.loop(0, part // TILE)
        def _(i, b=b):
            cols = pl.ds(pl.multiple_of(b * part + i * TILE, TILE), TILE)
            wd[:, cols] = dot(hid[...], dys[:, cols], 0, 0).astype(BF16)

        if b > 0:
            forward(*events.pop(0))
        pltpu.make_async_copy(x.at[:, band], wgu.at[:, slot], xload.at[b]).wait()

        for m, out in enumerate((wg, wu)):

            @pl.loop(0, hidden // TILE)
            def _(i, m=m, out=out, band=band, slot=slot):
                cols = pl.ds(pl.multiple_of(i * TILE, TILE), TILE)
                from_cols = pl.ds(pl.multiple_of(m * hidden + i * TILE, TILE), TILE)
                out[band, cols] = dot(wgu[:, slot], dgu[:, from_cols], 0, 0).astype(BF16)

            if m == 0:
                forward(*events.pop(0))
        if b + 2 < PIECES:
            load_x(b + 2)

    while events:
        forward(*events.pop(0))

    for q in range(PIECES):
        for s, h in units:
            if s >= chips - 2:
                pair(s, h, q).wait_send()
            if s < chips - 1:
                for d in (0, 1):
                    reduce(d, s, h, q).wait_send()
        for d in (0, 1):
            for hops in range(chips - 1):
                gather(d, hops, q).wait_send()
            for hops in range(chips):
                share(d, hops, q).wait_send()
                share(d, hops, q).wait_recv()


def store(*refs):
    n = (len(refs) - 1) // 2
    sems = refs[-1]
    for i, (src, dst) in enumerate(zip(refs[:n], refs[n:-1])):
        size = src.shape[0] // PIECES
        for p in range(PIECES):
            at = pl.ds(p * size, size)
            pltpu.make_async_copy(src.at[at], dst.at[at], sems.at[i]).start()
    for i, (src, dst) in enumerate(zip(refs[:n], refs[n:-1])):
        pltpu.make_async_copy(src, dst, sems.at[i]).wait()


def solution(mesh):
    chips = mesh.shape["tp"] // 2

    def step(x, dy, gate, up, w_gate, w_up, w_down):
        rows, width = x.shape
        hidden = gate.shape[1]
        block = rows // (4 * chips)
        shapes = ((rows, width), w_gate.shape, w_up.shape, w_down.shape)
        dma = pltpu.SemaphoreType.DMA
        outs = pl.pallas_call(
            functools.partial(work, chips),
            name="work",
            out_shape=[pltpu.VMEM(s, BF16) for s in shapes],
            in_specs=[ANY] * 7,
            out_specs=[VMEM] * 4,
            scratch_shapes=[
                pltpu.VMEM((chips, 2 * block, width), F32),
                pltpu.VMEM((chips, 2 * block, width), BF16),
                pltpu.VMEM((2, chips - 1, block, width), BF16),
                pltpu.VMEM((2, 2 * block, width), BF16),
                pltpu.VMEM((rows, width), BF16),
                pltpu.VMEM((rows, 2 * hidden), BF16),
                pltpu.VMEM((rows, hidden), BF16),
                pltpu.VMEM((2, 4 * block, hidden), BF16),
                pltpu.VMEM((2, 4 * block, hidden), BF16),
                pltpu.VMEM((width, 2 * hidden), BF16),
                dma((3, chips + 1)),
                dma((3, PIECES)),
                dma((PIECES,)),
                dma((chips + 1, PIECES)),
                dma((chips + 1, PIECES)),
                dma((2, chips, PIECES)),
                dma((2, chips, PIECES)),
                dma((2, chips - 1, PIECES)),
                dma((2, chips - 1, PIECES)),
                dma((2, chips, PIECES)),
                dma((2, chips, PIECES)),
            ],
            compiler_params=pltpu.CompilerParams(
                collective_id=0, has_side_effects=True, vmem_limit_bytes=46 * 2**20
            ),
        )(x, dy, gate, up, w_gate, w_up, w_down)
        return pl.pallas_call(
            store,
            name="store",
            out_shape=[jax.ShapeDtypeStruct(s, BF16) for s in shapes],
            in_specs=[VMEM] * 4,
            out_specs=[ANY] * 4,
            scratch_shapes=[dma((4,))],
            compiler_params=pltpu.CompilerParams(vmem_limit_bytes=2**20),
        )(*(pltpu.with_memory_space_constraint(o, pltpu.VMEM) for o in outs))

    tokens, columns, down = P("dp", None), P(None, "tp"), P("tp", None)
    return jax.shard_map(
        step,
        mesh=mesh,
        in_specs=(tokens, tokens, P("dp", "tp"), P("dp", "tp"), columns, columns, down),
        out_specs=(tokens, P("dp", "tp"), P("dp", "tp"), P(("dp", "tp"), None)),
        check_vma=False,
    )
```

```python
import functools

import jax
import jax.numpy as jnp
from jax import lax
from jax.experimental import pallas as pl
from jax.experimental.pallas import tpu as pltpu
from jax.sharding import PartitionSpec as P

BF16, F32 = jnp.bfloat16, jnp.float32
ANY = pl.BlockSpec(memory_space=pl.ANY)
VMEM = pl.BlockSpec(memory_space=pltpu.VMEM)
PIECES = 4
TILE = 256


def dot(a, b, a_dim, b_dim):
    return lax.dot_general(a, b, (((a_dim,), (b_dim,)), ((), ())), preferred_element_type=F32)


def work(
    chips, x, dy, gate, up, w_gate, w_up, w_down, dx, wg, wu, wd,
    own, got, ring, mate, dys, dgu, hid, gs, us, wgu,
    load, wload, xload, pair_s, pair_r, rs_s, rs_r, ag_s, ag_r, fin_s, fin_r,
):
    rows, width = dx.shape
    hidden = wd.shape[0]
    block = rows // (4 * chips)
    part = width // PIECES
    t = lax.axis_index("tp")
    k, c = t // 2, t % 2
    around = [k] + [(k + i) % chips for i in range(1, chips)]
    right = {"tp": around[1] * 2 + c}
    left = {"tp": around[-1] * 2 + c}
    partner = {"tp": k * 2 + 1 - c}
    ways = (right, left)

    def origin(d, hops):
        return around[-hops] if d == 0 else around[hops]

    def row(chunk, d, core):
        return pl.multiple_of((chunk * 4 + d * 2 + core) * block, block)

    units = [(0, 0), (0, 1)] + [(s, 0) for s in range(1, chips)]

    def high(s):
        return block // 2 if s == 0 else block

    def halves(s):
        return (0, 1) if s == 0 else (0,)

    def number(s, h):
        return units.index((s, h))

    def begin(s, h):
        return 4 * (s * block + h * high(s))

    def segments(s, h):
        todo = [around[-1 - s], around[(1 + s) % chips]]
        return [row(todo[d], d, core) + h * high(s) for core in (c, 1 - c) for d in (0, 1)]

    def load_dy(s, h):
        n = high(s)
        for i, r in enumerate(segments(s, h)):
            pltpu.make_async_copy(
                dy.at[pl.ds(r, n)], dys.at[pl.ds(begin(s, h) + i * n, n)], load.at[0, number(s, h)]
            ).start()

    def load_act(s, h):
        n = high(s)
        for i, r in enumerate(segments(s, h)):
            for m, (src, dst) in enumerate(((gate, gs), (up, us))):
                pltpu.make_async_copy(
                    src.at[pl.ds(r, n)],
                    dst.at[s % 2, pl.ds((h * 4 + i) * n, n)],
                    load.at[1 + m, number(s, h)],
                ).start()

    def load_x(b):
        for s, h in units:
            n = high(s)
            for i, r in enumerate(segments(s, h)):
                pltpu.make_async_copy(
                    x.at[pl.ds(r, n), pl.ds(b * part, part)],
                    wgu.at[pl.ds(begin(s, h) + i * n, n), pl.ds(b % 2 * part, part)],
                    xload.at[b],
                ).start()

    def weights(q):
        band = pl.ds(q * part, part)
        return [
            pltpu.make_async_copy(src.at[band], wgu.at[band, pl.ds(m * hidden, hidden)], wload.at[m, q])
            for m, src in enumerate((w_gate, w_up))
        ]

    def start(copies):
        for copy in copies:
            copy.start(priority=1)

    def weights_down(i):
        n = TILE // PIECES
        for j in range(PIECES):
            band = pl.ds(i * TILE + j * n, n)
            pltpu.make_async_copy(w_down.at[band], wd.at[band], wload.at[2, i]).start()

    def wait_weights_down(i):
        band = pl.ds(i * TILE, TILE)
        pltpu.make_async_copy(w_down.at[band], wd.at[band], wload.at[2, i]).wait()

    load_act(0, 0)
    load_dy(0, 0)
    for i in range(hidden // TILE):
        weights_down(i)
    start(weights(0))

    barrier = pltpu.get_barrier_semaphore()
    for other in (right, left, partner):
        pl.semaphore_signal(barrier, inc=1, device_id=other)

    def remote(src, dst, send, recv, to):
        return pltpu.make_async_remote_copy(src_ref=src, dst_ref=dst, send_sem=send, recv_sem=recv, device_id=to)

    def sent(like, sem):
        pltpu.make_async_copy(like, like, sem).wait()

    def pair(s, h, q):
        at = (pl.ds(h * 2 * high(s), 2 * high(s)), pl.ds(q * part, part))
        u = number(s, h)
        return remote(mate.at[s % 2, *at], got.at[s, *at], pair_s.at[s], pair_r.at[u, q], partner)

    def reduce(d, s, h, q):
        cols = pl.ds(q * part, part)
        n, u = high(s), number(s, h)
        return remote(
            got.at[s, pl.ds((h * 2 + d) * n, n), cols],
            ring.at[d, s, pl.ds(h * n, n), cols],
            rs_s.at[0],
            rs_r.at[d, u, q],
            ways[d],
        )

    def gather(d, hops, q):
        at = dx.at[pl.ds(row(origin(d, hops), d, c), block), pl.ds(q * part, part)]
        return remote(at, at, ag_s.at[0], ag_r.at[d, hops, q], ways[d])

    def share(d, hops, q):
        at = dx.at[pl.ds(row(origin(d, hops), d, c), block), pl.ds(q * part, part)]
        return remote(at, at, fin_s.at[0], fin_r.at[0], partner)

    def pass_on(s, h, q):
        cols = pl.ds(q * part, part)
        n = high(s)
        pair(s, h, q).wait_recv()
        for d in (0, 1):
            band = pl.ds((h * 2 + d) * n, n)
            total = own[s, band, cols] + got[s, band, cols].astype(F32)
            if s > 0:
                for before in halves(s - 1):
                    reduce(d, s - 1, before, q).wait_recv()
                total = total + ring[d, s - 1, :, cols].astype(F32)
            if s < chips - 1:
                got[s, band, cols] = total.astype(BF16)
            else:
                dx[pl.ds(row(k, d, c), block), cols] = total.astype(BF16)
        for d in (0, 1):
            if s < chips - 1:
                reduce(d, s, h, q).start()
            else:
                gather(d, 0, q).start()
        if s == chips - 1:
            for d in (0, 1):
                share(d, 0, q).start()

    def forward(hops, q):
        for d in (0, 1):
            gather(d, hops - 1, q).wait_recv()
            if hops < chips - 1:
                gather(d, hops, q).start()
            share(d, hops, q).start()

    waiting = []
    for s, h in units:
        n = high(s)
        here = pl.ds(begin(s, h), 4 * n)
        there = pl.ds(h * 4 * n, 4 * n)
        u = number(s, h)

        def gates(i, s=s, here=here, there=there):
            cols = pl.ds(pl.multiple_of(i * TILE, TILE), TILE)
            g = gs[s % 2, there, cols].astype(F32)
            v = us[s % 2, there, cols].astype(F32)
            sig = lax.logistic(g)
            silu = g * sig
            hid[here, cols] = (silu * v).astype(BF16)
            return silu, sig + g * (sig * (1.0 - sig)), v

        def back(i, silu, slope, v, here=here):
            cols = pl.ds(pl.multiple_of(i * TILE, TILE), TILE)
            up_cols = pl.ds(pl.multiple_of(hidden + i * TILE, TILE), TILE)
            dh = dot(dys[here], wd[cols, :], 1, 1)
            dgu[here, cols] = (dh * v * slope).astype(BF16)
            dgu[here, up_cols] = (dh * silu).astype(BF16)

        for m, (src, dst) in enumerate(((gate, gs), (up, us))):
            pltpu.make_async_copy(src.at[pl.ds(0, 4 * n)], dst.at[s % 2, there], load.at[1 + m, u]).wait()
        if s == 0:
            for i in range(hidden // TILE):
                silu, slope, _ = gates(i)
                own[chips - 1, pl.ds(0, 4 * n), pl.ds(i * TILE, TILE)] = silu
                own[chips - 1, pl.ds(0, 4 * n), pl.ds(hidden + i * TILE, TILE)] = slope
            while waiting:
                pass_on(*waiting.pop(0))
            pltpu.make_async_copy(dy.at[pl.ds(0, 4 * n)], dys.at[here], load.at[0, u]).wait()
            if u == 0:
                for i in range(hidden // TILE):
                    wait_weights_down(i)
                start(weights(1))
            silu = own[chips - 1, pl.ds(0, 4 * n), pl.ds(0, hidden)]
            slope = own[chips - 1, pl.ds(0, 4 * n), pl.ds(hidden, hidden)]
            dh = dot(dys[here], wd[...], 1, 1)
            dgu[here, pl.ds(0, hidden)] = (dh * us[0, there, :].astype(F32) * slope).astype(BF16)
            dgu[here, pl.ds(hidden, hidden)] = (dh * silu).astype(BF16)
            if u == 0:
                for q in range(2, PIECES):
                    start(weights(q))
        else:
            pltpu.make_async_copy(dy.at[pl.ds(0, 4 * n)], dys.at[here], load.at[0, u]).wait()
            back(0, *gates(0))
            while waiting:
                pass_on(*waiting.pop(0))
            pl.loop(1, hidden // TILE)(lambda i: back(i, *gates(i)))
        if u + 1 < len(units):
            load_dy(*units[u + 1])
            load_act(*units[u + 1])

        for q in range(PIECES):
            if u == 0:
                for copy in weights(q):
                    copy.wait()
            if s >= 2 and q == 0:
                sent(got.at[0], pair_s.at[s - 2])
            cols = pl.ds(q * part, part)
            v = dot(dgu[here, :], wgu[cols, :], 1, 1)
            mate[s % 2, pl.ds(h * 2 * n, 2 * n), cols] = v[2 * n :].astype(BF16)
            if u == 0 and q == 0:
                pl.semaphore_wait(barrier, 3)
            pair(s, h, q).start()
            own[s, pl.ds(h * 2 * n, 2 * n), cols] = v[: 2 * n]
            waiting.append((s, h, q))
            while len(waiting) > (2 if s == 0 else 1):
                pass_on(*waiting.pop(0))
        if (s, h) == units[-1]:
            load_x(0)
            load_x(1)
    while waiting:
        pass_on(*waiting.pop(0))

    events = [(hops, q) for hops in range(1, chips) for q in range(PIECES)]

    for b in range(PIECES):
        band = pl.ds(b * part, part)
        slot = pl.ds(b % 2 * part, part)

        @pl.loop(0, part // TILE)
        def _(i, b=b):
            cols = pl.ds(pl.multiple_of(b * part + i * TILE, TILE), TILE)
            wd[:, cols] = dot(hid[...], dys[:, cols], 0, 0).astype(BF16)

        if b > 0:
            forward(*events.pop(0))
        pltpu.make_async_copy(x.at[:, band], wgu.at[:, slot], xload.at[b]).wait()

        for m, out in enumerate((wg, wu)):

            @pl.loop(0, hidden // TILE)
            def _(i, m=m, out=out, band=band, slot=slot):
                cols = pl.ds(pl.multiple_of(i * TILE, TILE), TILE)
                from_cols = pl.ds(pl.multiple_of(m * hidden + i * TILE, TILE), TILE)
                out[band, cols] = dot(wgu[:, slot], dgu[:, from_cols], 0, 0).astype(BF16)

            if m == 0:
                forward(*events.pop(0))
        if b + 2 < PIECES:
            load_x(b + 2)

    while events:
        forward(*events.pop(0))

    for s in range(max(chips - 2, 0), chips):
        sent(got.at[0], pair_s.at[s])
    sent(dx.at[pl.ds(0, 2 * (chips - 1) * block)], rs_s.at[0])
    sent(dx.at[pl.ds(0, 2 * (chips - 1) * block)], ag_s.at[0])
    sent(dx.at[pl.ds(0, 2 * chips * block)], fin_s.at[0])
    sent(dx.at[pl.ds(0, 2 * chips * block)], fin_r.at[0])


def store(*refs):
    n = (len(refs) - 1) // 2
    sems = refs[-1]
    for i, (src, dst) in enumerate(zip(refs[:n], refs[n:-1])):
        size = src.shape[0] // PIECES
        for p in range(PIECES):
            at = pl.ds(p * size, size)
            pltpu.make_async_copy(src.at[at], dst.at[at], sems.at[i]).start()
    for i, (src, dst) in enumerate(zip(refs[:n], refs[n:-1])):
        pltpu.make_async_copy(src, dst, sems.at[i]).wait()


def solution(mesh):
    chips = mesh.shape["tp"] // 2

    def step(x, dy, gate, up, w_gate, w_up, w_down):
        rows, width = x.shape
        hidden = gate.shape[1]
        block = rows // (4 * chips)
        shapes = ((rows, width), w_gate.shape, w_up.shape, w_down.shape)
        dma = pltpu.SemaphoreType.DMA
        outs = pl.pallas_call(
            functools.partial(work, chips),
            name="work",
            out_shape=[pltpu.VMEM(s, BF16) for s in shapes],
            in_specs=[ANY] * 7,
            out_specs=[VMEM] * 4,
            scratch_shapes=[
                pltpu.VMEM((chips, 2 * block, width), F32),
                pltpu.VMEM((chips, 2 * block, width), BF16),
                pltpu.VMEM((2, chips - 1, block, width), BF16),
                pltpu.VMEM((2, 2 * block, width), BF16),
                pltpu.VMEM((rows, width), BF16),
                pltpu.VMEM((rows, 2 * hidden), BF16),
                pltpu.VMEM((rows, hidden), BF16),
                pltpu.VMEM((2, 4 * block, hidden), BF16),
                pltpu.VMEM((2, 4 * block, hidden), BF16),
                pltpu.VMEM((width, 2 * hidden), BF16),
                dma((3, chips + 1)),
                dma((3, PIECES)),
                dma((PIECES,)),
                dma((chips,)),
                dma((chips + 1, PIECES)),
                dma((1,)),
                dma((2, chips, PIECES)),
                dma((1,)),
                dma((2, chips - 1, PIECES)),
                dma((1,)),
                dma((1,)),
            ],
            compiler_params=pltpu.CompilerParams(
                collective_id=0, has_side_effects=True, vmem_limit_bytes=46 * 2**20
            ),
        )(x, dy, gate, up, w_gate, w_up, w_down)
        return pl.pallas_call(
            store,
            name="store",
            out_shape=[jax.ShapeDtypeStruct(s, BF16) for s in shapes],
            in_specs=[VMEM] * 4,
            out_specs=[ANY] * 4,
            scratch_shapes=[dma((4,))],
            compiler_params=pltpu.CompilerParams(vmem_limit_bytes=2**20),
        )(*(pltpu.with_memory_space_constraint(o, pltpu.VMEM) for o in outs))

    tokens, columns, down = P("dp", None), P(None, "tp"), P("tp", None)
    return jax.shard_map(
        step,
        mesh=mesh,
        in_specs=(tokens, tokens, P("dp", "tp"), P("dp", "tp"), columns, columns, down),
        out_specs=(tokens, P("dp", "tp"), P("dp", "tp"), P(("dp", "tp"), None)),
        check_vma=False,
    )
```

```python
import functools

import jax
import jax.numpy as jnp
from jax import lax
from jax.experimental import pallas as pl
from jax.experimental.pallas import tpu as pltpu
from jax.sharding import PartitionSpec as P

BF16, F32 = jnp.bfloat16, jnp.float32
ANY = pl.BlockSpec(memory_space=pl.ANY)
VMEM = pl.BlockSpec(memory_space=pltpu.VMEM)
PIECES = 4
SPLIT = 2
TILE = 256


def dot(a, b, a_dim, b_dim):
    return lax.dot_general(a, b, (((a_dim,), (b_dim,)), ((), ())), preferred_element_type=F32)


def work(
    chips, x, dy, gate, up, w_gate, w_up, w_down, dx, wg, wu, wd,
    own, got, ring, mate, dys, dgu, hid, gs, us, wgu,
    load, wload, xload, pair_s, pair_r, rs_s, rs_r, ag_s, ag_r, fin_s, fin_r,
):
    rows, width = dx.shape
    hidden = wd.shape[0]
    block = rows // (4 * chips)
    part = width // PIECES
    t = lax.axis_index("tp")
    k, c = t // 2, t % 2
    around = [k] + [(k + i) % chips for i in range(1, chips)]
    right = {"tp": around[1] * 2 + c}
    left = {"tp": around[-1] * 2 + c}
    partner = {"tp": k * 2 + 1 - c}
    ways = (right, left)

    def origin(d, hops):
        return around[-hops] if d == 0 else around[hops]

    def row(chunk, d, core):
        return pl.multiple_of((chunk * 4 + d * 2 + core) * block, block)

    split = min(SPLIT, chips - 1)
    units = [(s, h) for s in range(split) for h in (0, 1)] + [(s, 0) for s in range(split, chips)]

    quarters, halves_of = [(q * part, part) for q in range(PIECES)], [(0, width // 2), (width // 2, width // 2)]
    pair_cuts = [[(0, part // 2), (part // 2, part // 2), *quarters[1:]]] + [quarters] * (len(units) - 1)
    sum_cuts = pair_cuts[: 2 * split] + [halves_of if s > 2 else quarters for s in range(split, chips)]
    gather_cuts = [halves_of] * (chips - 2) + [quarters]

    def within(cut, cuts):
        return [i for i, (a, n) in enumerate(cuts) if cut[0] <= a and a + n <= cut[0] + cut[1]]

    def high(s):
        return block // 2 if s < split else block

    def halves(s):
        return (0, 1) if s < split else (0,)

    def number(s, h):
        return units.index((s, h))

    def begin(s, h):
        return 4 * (s * block + h * high(s))

    def segments(s, h):
        todo = [around[-1 - s], around[(1 + s) % chips]]
        return [row(todo[d], d, core) + h * high(s) for core in (c, 1 - c) for d in (0, 1)]

    def load_dy(s, h):
        n = high(s)
        for i, r in enumerate(segments(s, h)):
            pltpu.make_async_copy(
                dy.at[pl.ds(r, n)], dys.at[pl.ds(begin(s, h) + i * n, n)], load.at[0, number(s, h)]
            ).start()

    def load_act(s, h):
        n = high(s)
        for i, r in enumerate(segments(s, h)):
            for m, (src, dst) in enumerate(((gate, gs), (up, us))):
                pltpu.make_async_copy(
                    src.at[pl.ds(r, n)],
                    dst.at[s % 2, pl.ds((h * 4 + i) * n, n)],
                    load.at[1 + m, number(s, h)],
                ).start()

    def load_x(b):
        for s, h in units:
            n = high(s)
            for i, r in enumerate(segments(s, h)):
                pltpu.make_async_copy(
                    x.at[pl.ds(r, n), pl.ds(b * part, part)],
                    wgu.at[pl.ds(begin(s, h) + i * n, n), pl.ds(b % 2 * part, part)],
                    xload.at[b],
                ).start()

    def weights(q):
        band = pl.ds(q * part, part)
        return [
            pltpu.make_async_copy(src.at[band], wgu.at[band, pl.ds(m * hidden, hidden)], wload.at[m, q])
            for m, src in enumerate((w_gate, w_up))
        ]

    def start(copies):
        for copy in copies:
            copy.start(priority=1)

    def weights_down(i):
        n = TILE // PIECES
        for j in range(PIECES):
            band = pl.ds(i * TILE + j * n, n)
            pltpu.make_async_copy(w_down.at[band], wd.at[band], wload.at[2, i]).start()

    def wait_weights_down(i):
        band = pl.ds(i * TILE, TILE)
        pltpu.make_async_copy(w_down.at[band], wd.at[band], wload.at[2, i]).wait()

    load_act(0, 0)
    load_dy(0, 0)
    for i in range(hidden // TILE):
        weights_down(i)
    start(weights(0))

    barrier = pltpu.get_barrier_semaphore()
    for other in (right, left, partner):
        pl.semaphore_signal(barrier, inc=1, device_id=other)

    def remote(src, dst, send, recv, to):
        return pltpu.make_async_remote_copy(src_ref=src, dst_ref=dst, send_sem=send, recv_sem=recv, device_id=to)

    def sent(like, sem):
        pltpu.make_async_copy(like, like, sem).wait()

    def pair(s, h, i):
        u = number(s, h)
        at = (pl.ds(h * 2 * high(s), 2 * high(s)), pl.ds(*pair_cuts[u][i]))
        return remote(mate.at[s % 2, *at], got.at[s, *at], pair_s.at[s], pair_r.at[u, i], partner)

    def reduce(d, s, h, i):
        n, u = high(s), number(s, h)
        cols = pl.ds(*sum_cuts[u][i])
        return remote(
            got.at[s, pl.ds((h * 2 + d) * n, n), cols],
            ring.at[d, s, pl.ds(h * n, n), cols],
            rs_s.at[0],
            rs_r.at[d, u, i],
            ways[d],
        )

    def gather(d, hops, i):
        at = dx.at[pl.ds(row(origin(d, hops), d, c), block), pl.ds(*gather_cuts[hops][i])]
        return remote(at, at, ag_s.at[0], ag_r.at[d, hops, i], ways[d])

    def share(d, hops, cut):
        at = dx.at[pl.ds(row(origin(d, hops), d, c), block), pl.ds(*cut)]
        return remote(at, at, fin_s.at[0], fin_r.at[0], partner)

    def pass_on(s, h, i):
        n, u = high(s), number(s, h)
        cut = sum_cuts[u][i]
        cols = pl.ds(*cut)
        for j in within(cut, pair_cuts[u]):
            pair(s, h, j).wait_recv()
        for d in (0, 1):
            band = pl.ds((h * 2 + d) * n, n)
            total = own[s, band, cols] + got[s, band, cols].astype(F32)
            if s > 0:
                for before in (h,) if s < split else halves(s - 1):
                    for j in within(cut, sum_cuts[number(s - 1, before)]):
                        reduce(d, s - 1, before, j).wait_recv()
                total = total + ring[d, s - 1, pl.ds(h * n, n), cols].astype(F32)
            if s < chips - 1:
                got[s, band, cols] = total.astype(BF16)
            else:
                dx[pl.ds(row(k, d, c), block), cols] = total.astype(BF16)
        for d in (0, 1):
            if s < chips - 1:
                reduce(d, s, h, i).start()
            else:
                for j in within(cut, gather_cuts[0]):
                    gather(d, 0, j).start()
        if s == chips - 1:
            for d in (0, 1):
                share(d, 0, cut).start()

    def forward(hops, i):
        cut = gather_cuts[hops - 1][i]
        for d in (0, 1):
            gather(d, hops - 1, i).wait_recv()
            if hops < chips - 1:
                for j in within(cut, gather_cuts[hops]):
                    gather(d, hops, j).start()
            share(d, hops, cut).start()

    waiting = []

    def flush(lag=0):
        while waiting and begun[0] - waiting[0][1] >= lag:
            pass_on(*waiting.pop(0)[0])

    begun = [0]
    for s, h in units:
        n = high(s)
        here = pl.ds(begin(s, h), 4 * n)
        there = pl.ds(h * 4 * n, 4 * n)
        u = number(s, h)

        def gates(i, s=s, here=here, there=there):
            cols = pl.ds(pl.multiple_of(i * TILE, TILE), TILE)
            g = gs[s % 2, there, cols].astype(F32)
            v = us[s % 2, there, cols].astype(F32)
            sig = lax.logistic(g)
            silu = g * sig
            hid[here, cols] = (silu * v).astype(BF16)
            return silu, sig + g * (sig * (1.0 - sig)), v

        def back(i, silu, slope, v, here=here):
            cols = pl.ds(pl.multiple_of(i * TILE, TILE), TILE)
            up_cols = pl.ds(pl.multiple_of(hidden + i * TILE, TILE), TILE)
            dh = dot(dys[here], wd[cols, :], 1, 1)
            dgu[here, cols] = (dh * v * slope).astype(BF16)
            dgu[here, up_cols] = (dh * silu).astype(BF16)

        for m, (src, dst) in enumerate(((gate, gs), (up, us))):
            pltpu.make_async_copy(src.at[pl.ds(0, 4 * n)], dst.at[s % 2, there], load.at[1 + m, u]).wait()
        if s < split:
            for i in range(hidden // TILE):
                silu, slope, _ = gates(i)
                own[chips - 1, pl.ds(0, 4 * n), pl.ds(i * TILE, TILE)] = silu
                own[chips - 1, pl.ds(0, 4 * n), pl.ds(hidden + i * TILE, TILE)] = slope
            flush()
            pltpu.make_async_copy(dy.at[pl.ds(0, 4 * n)], dys.at[here], load.at[0, u]).wait()
            if u == 0:
                for i in range(hidden // TILE):
                    wait_weights_down(i)
                start(weights(1))
            silu = own[chips - 1, pl.ds(0, 4 * n), pl.ds(0, hidden)]
            slope = own[chips - 1, pl.ds(0, 4 * n), pl.ds(hidden, hidden)]
            dh = dot(dys[here], wd[...], 1, 1)
            dgu[here, pl.ds(0, hidden)] = (dh * us[s % 2, there, :].astype(F32) * slope).astype(BF16)
            dgu[here, pl.ds(hidden, hidden)] = (dh * silu).astype(BF16)
            if u == 0:
                for q in range(2, PIECES):
                    start(weights(q))
        else:
            pltpu.make_async_copy(dy.at[pl.ds(0, 4 * n)], dys.at[here], load.at[0, u]).wait()
            back(0, *gates(0))
            flush()
            pl.loop(1, hidden // TILE)(lambda i: back(i, *gates(i)))
        if u + 1 < len(units):
            load_dy(*units[u + 1])
            load_act(*units[u + 1])

        for i, cut in enumerate(pair_cuts[u]):
            if u == 0 and cut[0] % part == 0:
                for copy in weights(cut[0] // part):
                    copy.wait()
            if s >= 2 and h == 0 and i == 0:
                sent(got.at[0], pair_s.at[s - 2])
            cols = pl.ds(*cut)
            v = dot(dgu[here, :], wgu[cols, :], 1, 1)
            mate[s % 2, pl.ds(h * 2 * n, 2 * n), cols] = v[2 * n :].astype(BF16)
            if u == 0 and i == 0:
                pl.semaphore_wait(barrier, 3)
            pair(s, h, i).start()
            own[s, pl.ds(h * 2 * n, 2 * n), cols] = v[: 2 * n]
            begun[0] += 1
            for j, whole in enumerate(sum_cuts[u]):
                if within(whole, pair_cuts[u])[-1] == i:
                    waiting.append(((s, h, j), begun[0]))
            flush(2 if s < split else 1)
        if (s, h) == units[-1]:
            load_x(0)
            load_x(1)
    flush()

    events = [(hops, i) for hops in range(1, chips) for i in range(len(gather_cuts[hops - 1]))]

    for b in range(PIECES):
        band = pl.ds(b * part, part)
        slot = pl.ds(b % 2 * part, part)

        @pl.loop(0, part // TILE)
        def _(i, b=b):
            cols = pl.ds(pl.multiple_of(b * part + i * TILE, TILE), TILE)
            wd[:, cols] = dot(hid[...], dys[:, cols], 0, 0).astype(BF16)

        if b == PIECES - 1:
            forward(*events.pop(0))
        pltpu.make_async_copy(x.at[:, band], wgu.at[:, slot], xload.at[b]).wait()

        for m, out in enumerate((wg, wu)):

            @pl.loop(0, hidden // TILE)
            def _(i, m=m, out=out, band=band, slot=slot):
                cols = pl.ds(pl.multiple_of(i * TILE, TILE), TILE)
                from_cols = pl.ds(pl.multiple_of(m * hidden + i * TILE, TILE), TILE)
                out[band, cols] = dot(wgu[:, slot], dgu[:, from_cols], 0, 0).astype(BF16)

            if (b, m) in ((0, 1), (1, 0), (2, 0)):
                forward(*events.pop(0))
        if b + 2 < PIECES:
            load_x(b + 2)

    while events:
        forward(*events.pop(0))

    for s in range(max(chips - 2, 0), chips):
        sent(got.at[0], pair_s.at[s])
    sent(dx.at[pl.ds(0, 2 * (chips - 1) * block)], rs_s.at[0])
    sent(dx.at[pl.ds(0, 2 * (chips - 1) * block)], ag_s.at[0])
    sent(dx.at[pl.ds(0, 2 * chips * block)], fin_s.at[0])
    sent(dx.at[pl.ds(0, 2 * chips * block)], fin_r.at[0])


def store(*refs):
    n = (len(refs) - 1) // 2
    sems = refs[-1]
    for i, (src, dst) in enumerate(zip(refs[:n], refs[n:-1])):
        size = src.shape[0] // PIECES
        for p in range(PIECES):
            at = pl.ds(p * size, size)
            pltpu.make_async_copy(src.at[at], dst.at[at], sems.at[i]).start()
    for i, (src, dst) in enumerate(zip(refs[:n], refs[n:-1])):
        pltpu.make_async_copy(src, dst, sems.at[i]).wait()


def solution(mesh):
    chips = mesh.shape["tp"] // 2

    def step(x, dy, gate, up, w_gate, w_up, w_down):
        rows, width = x.shape
        hidden = gate.shape[1]
        block = rows // (4 * chips)
        shapes = ((rows, width), w_gate.shape, w_up.shape, w_down.shape)
        dma = pltpu.SemaphoreType.DMA
        outs = pl.pallas_call(
            functools.partial(work, chips),
            name="work",
            out_shape=[pltpu.VMEM(s, BF16) for s in shapes],
            in_specs=[ANY] * 7,
            out_specs=[VMEM] * 4,
            scratch_shapes=[
                pltpu.VMEM((chips, 2 * block, width), F32),
                pltpu.VMEM((chips, 2 * block, width), BF16),
                pltpu.VMEM((2, chips - 1, block, width), BF16),
                pltpu.VMEM((2, 2 * block, width), BF16),
                pltpu.VMEM((rows, width), BF16),
                pltpu.VMEM((rows, 2 * hidden), BF16),
                pltpu.VMEM((rows, hidden), BF16),
                pltpu.VMEM((2, 4 * block, hidden), BF16),
                pltpu.VMEM((2, 4 * block, hidden), BF16),
                pltpu.VMEM((width, 2 * hidden), BF16),
                dma((3, chips + SPLIT)),
                dma((3, PIECES)),
                dma((PIECES,)),
                dma((chips,)),
                dma((chips + SPLIT, PIECES + 1)),
                dma((1,)),
                dma((2, chips + SPLIT - 1, PIECES + 1)),
                dma((1,)),
                dma((2, chips - 1, PIECES)),
                dma((1,)),
                dma((1,)),
            ],
            compiler_params=pltpu.CompilerParams(
                collective_id=0, has_side_effects=True, vmem_limit_bytes=46 * 2**20
            ),
        )(x, dy, gate, up, w_gate, w_up, w_down)
        return pl.pallas_call(
            store,
            name="store",
            out_shape=[jax.ShapeDtypeStruct(s, BF16) for s in shapes],
            in_specs=[VMEM] * 4,
            out_specs=[ANY] * 4,
            scratch_shapes=[dma((4,))],
            compiler_params=pltpu.CompilerParams(vmem_limit_bytes=2**20),
        )(*(pltpu.with_memory_space_constraint(o, pltpu.VMEM) for o in outs))

    tokens, columns, down = P("dp", None), P(None, "tp"), P("tp", None)
    return jax.shard_map(
        step,
        mesh=mesh,
        in_specs=(tokens, tokens, P("dp", "tp"), P("dp", "tp"), columns, columns, down),
        out_specs=(tokens, P("dp", "tp"), P("dp", "tp"), P(("dp", "tp"), None)),
        check_vma=False,
    )
```

```python
import functools

import jax
import jax.numpy as jnp
from jax import lax
from jax.experimental import pallas as pl
from jax.experimental.pallas import tpu as pltpu
from jax.sharding import PartitionSpec as P

BF16, F32 = jnp.bfloat16, jnp.float32
ANY = pl.BlockSpec(memory_space=pl.ANY)
VMEM = pl.BlockSpec(memory_space=pltpu.VMEM)
PIECES = 4
SPLIT = 2
STORES = 16
TILE = 256


def dot(a, b, a_dim, b_dim):
    return lax.dot_general(a, b, (((a_dim,), (b_dim,)), ((), ())), preferred_element_type=F32)


def work(
    chips, x, dy, gate, up, w_gate, w_up, w_down, dx, wg, wu, wd,
    own, got, ring, mate, dys, dgu, hid, gs, us, wgu,
    load, wload, xload, pair_s, pair_r, rs_s, rs_r, ag_s, ag_r, fin_s, fin_r,
):
    rows, width = dx.shape
    hidden = wd.shape[0]
    block = rows // (4 * chips)
    part = width // PIECES
    t = lax.axis_index("tp")
    k, c = t // 2, t % 2
    around = [k] + [(k + i) % chips for i in range(1, chips)]
    right = {"tp": around[1] * 2 + c}
    left = {"tp": around[-1] * 2 + c}
    partner = {"tp": k * 2 + 1 - c}
    ways = (right, left)

    def origin(d, hops):
        return around[-hops] if d == 0 else around[hops]

    def row(chunk, d, core):
        return pl.multiple_of((chunk * 4 + d * 2 + core) * block, block)

    split = min(SPLIT, chips - 1)
    units = [(s, h) for s in range(split) for h in (0, 1)] + [(s, 0) for s in range(split, chips)]

    quarters, halves_of = [(q * part, part) for q in range(PIECES)], [(0, width // 2), (width // 2, width // 2)]
    pair_cuts = [[(0, part // 2), (part // 2, part // 2), *quarters[1:]]] + [quarters] * (len(units) - 1)
    sum_cuts = pair_cuts[: 2 * split] + [halves_of if s > 2 else quarters for s in range(split, chips)]
    last = [(0, 2 * part), (2 * part, part), (3 * part, part // 2), (3 * part + part // 2, part // 2)]
    gather_cuts = [halves_of] * (chips - 2) + [last]

    def within(cut, cuts):
        return [i for i, (a, n) in enumerate(cuts) if cut[0] <= a and a + n <= cut[0] + cut[1]]

    def high(s):
        return block // 2 if s < split else block

    def halves(s):
        return (0, 1) if s < split else (0,)

    def number(s, h):
        return units.index((s, h))

    def begin(s, h):
        return 4 * (s * block + h * high(s))

    def segments(s, h):
        todo = [around[-1 - s], around[(1 + s) % chips]]
        return [row(todo[d], d, core) + h * high(s) for core in (c, 1 - c) for d in (0, 1)]

    def load_dy(s, h):
        n = high(s)
        for i, r in enumerate(segments(s, h)):
            pltpu.make_async_copy(
                dy.at[pl.ds(r, n)], dys.at[pl.ds(begin(s, h) + i * n, n)], load.at[0, number(s, h)]
            ).start(priority=0 if (s, h) == (0, 0) else 1)

    def load_act(s, h):
        n = high(s)
        for i, r in enumerate(segments(s, h)):
            for m, (src, dst) in enumerate(((gate, gs), (up, us))):
                pltpu.make_async_copy(
                    src.at[pl.ds(r, n)],
                    dst.at[s % 2, pl.ds((h * 4 + i) * n, n)],
                    load.at[1 + m, number(s, h)],
                ).start(priority=0 if (s, h) == (0, 0) else 1)

    def load_x(b):
        for s, h in units:
            n = high(s)
            for i, r in enumerate(segments(s, h)):
                pltpu.make_async_copy(
                    x.at[pl.ds(r, n), pl.ds(b * part, part)],
                    wgu.at[pl.ds(begin(s, h) + i * n, n), pl.ds(b % 2 * part, part)],
                    xload.at[b],
                ).start(priority=1)

    def weights(q):
        band = pl.ds(q * part, part)
        return [
            pltpu.make_async_copy(src.at[band], wgu.at[band, pl.ds(m * hidden, hidden)], wload.at[m, q])
            for m, src in enumerate((w_gate, w_up))
        ]

    def start(copies):
        for copy in copies:
            copy.start(priority=1)

    def weights_down(i):
        n = TILE // PIECES
        for j in range(PIECES):
            band = pl.ds(i * TILE + j * n, n)
            pltpu.make_async_copy(w_down.at[band], wd.at[band], wload.at[2, i]).start()

    def wait_weights_down(i):
        band = pl.ds(i * TILE, TILE)
        pltpu.make_async_copy(w_down.at[band], wd.at[band], wload.at[2, i]).wait()

    load_act(0, 0)
    load_dy(0, 0)
    for i in range(hidden // TILE):
        weights_down(i)
    start(weights(0))

    barrier = pltpu.get_barrier_semaphore()
    for other in (right, left, partner):
        pl.semaphore_signal(barrier, inc=1, device_id=other)

    def remote(src, dst, send, recv, to):
        return pltpu.make_async_remote_copy(src_ref=src, dst_ref=dst, send_sem=send, recv_sem=recv, device_id=to)

    def sent(like, sem):
        pltpu.make_async_copy(like, like, sem).wait()

    def pair(s, h, i):
        u = number(s, h)
        at = (pl.ds(h * 2 * high(s), 2 * high(s)), pl.ds(*pair_cuts[u][i]))
        return remote(mate.at[s % 2, *at], got.at[s, *at], pair_s.at[s], pair_r.at[u, i], partner)

    def reduce(d, s, h, i):
        n, u = high(s), number(s, h)
        cols = pl.ds(*sum_cuts[u][i])
        return remote(
            got.at[s, pl.ds((h * 2 + d) * n, n), cols],
            ring.at[d, s, pl.ds(h * n, n), cols],
            rs_s.at[0],
            rs_r.at[d, u, i],
            ways[d],
        )

    def gather(d, hops, i):
        at = dx.at[pl.ds(row(origin(d, hops), d, c), block), pl.ds(*gather_cuts[hops][i])]
        return remote(at, at, ag_s.at[0], ag_r.at[d, hops, i], ways[d])

    def share(d, hops, cut):
        at = dx.at[pl.ds(row(origin(d, hops), d, c), block), pl.ds(*cut)]
        return remote(at, at, fin_s.at[0], fin_r.at[0], partner)

    def pass_on(s, h, i):
        n, u = high(s), number(s, h)
        cut = sum_cuts[u][i]
        cols = pl.ds(*cut)
        for j in within(cut, pair_cuts[u]):
            pair(s, h, j).wait_recv()
        for d in (0, 1):
            band = pl.ds((h * 2 + d) * n, n)
            total = own[s, band, cols] + got[s, band, cols].astype(F32)
            if s > 0:
                for before in (h,) if s < split else halves(s - 1):
                    for j in within(cut, sum_cuts[number(s - 1, before)]):
                        reduce(d, s - 1, before, j).wait_recv()
                total = total + ring[d, s - 1, pl.ds(h * n, n), cols].astype(F32)
            if s < chips - 1:
                got[s, band, cols] = total.astype(BF16)
            else:
                dx[pl.ds(row(k, d, c), block), cols] = total.astype(BF16)
        for d in (0, 1):
            if s < chips - 1:
                reduce(d, s, h, i).start()
            else:
                for j in within(cut, gather_cuts[0]):
                    gather(d, 0, j).start()
        if s == chips - 1:
            for d in (0, 1):
                share(d, 0, cut).start()

    def forward(hops, i):
        cut = gather_cuts[hops - 1][i]
        for d in (0, 1):
            gather(d, hops - 1, i).wait_recv()
            if hops < chips - 1:
                for j in within(cut, gather_cuts[hops]):
                    gather(d, hops, j).start()
            share(d, hops, cut).start()

    waiting = []

    def flush(lag=0):
        while waiting and begun[0] - waiting[0][1] >= lag:
            pass_on(*waiting.pop(0)[0])

    begun = [0]
    for s, h in units:
        n = high(s)
        here = pl.ds(begin(s, h), 4 * n)
        there = pl.ds(h * 4 * n, 4 * n)
        u = number(s, h)

        def gates(i, s=s, here=here, there=there):
            cols = pl.ds(pl.multiple_of(i * TILE, TILE), TILE)
            g = gs[s % 2, there, cols].astype(F32)
            v = us[s % 2, there, cols].astype(F32)
            sig = lax.logistic(g)
            silu = g * sig
            hid[here, cols] = (silu * v).astype(BF16)
            return silu, sig + g * (sig * (1.0 - sig)), v

        def back(i, silu, slope, v, here=here):
            cols = pl.ds(pl.multiple_of(i * TILE, TILE), TILE)
            up_cols = pl.ds(pl.multiple_of(hidden + i * TILE, TILE), TILE)
            dh = dot(dys[here], wd[cols, :], 1, 1)
            dgu[here, cols] = (dh * v * slope).astype(BF16)
            dgu[here, up_cols] = (dh * silu).astype(BF16)

        for m, (src, dst) in enumerate(((gate, gs), (up, us))):
            pltpu.make_async_copy(src.at[pl.ds(0, 4 * n)], dst.at[s % 2, there], load.at[1 + m, u]).wait()
        if s < split:
            for i in range(hidden // TILE):
                silu, slope, _ = gates(i)
                own[chips - 1, pl.ds(0, 4 * n), pl.ds(i * TILE, TILE)] = silu
                own[chips - 1, pl.ds(0, 4 * n), pl.ds(hidden + i * TILE, TILE)] = slope
            flush()
            pltpu.make_async_copy(dy.at[pl.ds(0, 4 * n)], dys.at[here], load.at[0, u]).wait()
            if u == 0:
                for i in range(hidden // TILE):
                    wait_weights_down(i)
                start(weights(1))
            silu = own[chips - 1, pl.ds(0, 4 * n), pl.ds(0, hidden)]
            slope = own[chips - 1, pl.ds(0, 4 * n), pl.ds(hidden, hidden)]
            dh = dot(dys[here], wd[...], 1, 1)
            dgu[here, pl.ds(0, hidden)] = (dh * us[s % 2, there, :].astype(F32) * slope).astype(BF16)
            dgu[here, pl.ds(hidden, hidden)] = (dh * silu).astype(BF16)
            if u == 0:
                for q in range(2, PIECES):
                    start(weights(q))
        else:
            pltpu.make_async_copy(dy.at[pl.ds(0, 4 * n)], dys.at[here], load.at[0, u]).wait()
            back(0, *gates(0))
            flush()
            pl.loop(1, hidden // TILE)(lambda i: back(i, *gates(i)))
        if u + 1 < len(units):
            load_dy(*units[u + 1])
            load_act(*units[u + 1])

        for i, cut in enumerate(pair_cuts[u]):
            if u == 0 and cut[0] % part == 0:
                for copy in weights(cut[0] // part):
                    copy.wait()
            if s >= 2 and h == 0 and i == 0:
                sent(got.at[0], pair_s.at[s - 2])
            cols = pl.ds(*cut)
            v = dot(dgu[here, :], wgu[cols, :], 1, 1)
            mate[s % 2, pl.ds(h * 2 * n, 2 * n), cols] = v[2 * n :].astype(BF16)
            if u == 0 and i == 0:
                pl.semaphore_wait(barrier, 3)
            pair(s, h, i).start()
            own[s, pl.ds(h * 2 * n, 2 * n), cols] = v[: 2 * n]
            begun[0] += 1
            for j, whole in enumerate(sum_cuts[u]):
                if within(whole, pair_cuts[u])[-1] == i:
                    waiting.append(((s, h, j), begun[0]))
            flush(2 if s < split else 1)
        if (s, h) == units[-1]:
            load_x(0)
            load_x(1)
    flush()

    events = [(hops, i) for hops in range(1, chips) for i in range(len(gather_cuts[hops - 1]))]

    for b in range(PIECES):
        band = pl.ds(b * part, part)
        slot = pl.ds(b % 2 * part, part)

        @pl.loop(0, part // TILE)
        def _(i, b=b):
            cols = pl.ds(pl.multiple_of(b * part + i * TILE, TILE), TILE)
            wd[:, cols] = dot(hid[...], dys[:, cols], 0, 0).astype(BF16)

        if b == PIECES - 1:
            forward(*events.pop(0))
        pltpu.make_async_copy(x.at[:, band], wgu.at[:, slot], xload.at[b]).wait()

        for m, out in enumerate((wg, wu)):

            @pl.loop(0, hidden // TILE)
            def _(i, m=m, out=out, band=band, slot=slot):
                cols = pl.ds(pl.multiple_of(i * TILE, TILE), TILE)
                from_cols = pl.ds(pl.multiple_of(m * hidden + i * TILE, TILE), TILE)
                out[band, cols] = dot(wgu[:, slot], dgu[:, from_cols], 0, 0).astype(BF16)

            if (b, m) in ((0, 1), (1, 0), (2, 0)):
                forward(*events.pop(0))
        if b + 2 < PIECES:
            load_x(b + 2)

    while events:
        forward(*events.pop(0))

    for s in range(max(chips - 2, 0), chips):
        sent(got.at[0], pair_s.at[s])
    sent(dx.at[pl.ds(0, 2 * (chips - 1) * block)], rs_s.at[0])
    sent(dx.at[pl.ds(0, 2 * (chips - 1) * block)], ag_s.at[0])
    sent(dx.at[pl.ds(0, 2 * chips * block)], fin_s.at[0])
    sent(dx.at[pl.ds(0, 2 * chips * block)], fin_r.at[0])


def store(*refs):
    n = (len(refs) - 1) // 2
    sems = refs[-1]
    for i, (src, dst) in enumerate(zip(refs[:n], refs[n:-1])):
        size = src.shape[0] // STORES
        for p in range(STORES):
            at = pl.ds(p * size, size)
            pltpu.make_async_copy(src.at[at], dst.at[at], sems.at[i]).start()
    for i, (src, dst) in enumerate(zip(refs[:n], refs[n:-1])):
        pltpu.make_async_copy(src, dst, sems.at[i]).wait()


def solution(mesh):
    chips = mesh.shape["tp"] // 2

    def step(x, dy, gate, up, w_gate, w_up, w_down):
        rows, width = x.shape
        hidden = gate.shape[1]
        block = rows // (4 * chips)
        shapes = ((rows, width), w_gate.shape, w_up.shape, w_down.shape)
        dma = pltpu.SemaphoreType.DMA
        outs = pl.pallas_call(
            functools.partial(work, chips),
            name="work",
            out_shape=[pltpu.VMEM(s, BF16) for s in shapes],
            in_specs=[ANY] * 7,
            out_specs=[VMEM] * 4,
            scratch_shapes=[
                pltpu.VMEM((chips, 2 * block, width), F32),
                pltpu.VMEM((chips, 2 * block, width), BF16),
                pltpu.VMEM((2, chips - 1, block, width), BF16),
                pltpu.VMEM((2, 2 * block, width), BF16),
                pltpu.VMEM((rows, width), BF16),
                pltpu.VMEM((rows, 2 * hidden), BF16),
                pltpu.VMEM((rows, hidden), BF16),
                pltpu.VMEM((2, 4 * block, hidden), BF16),
                pltpu.VMEM((2, 4 * block, hidden), BF16),
                pltpu.VMEM((width, 2 * hidden), BF16),
                dma((3, chips + SPLIT)),
                dma((3, PIECES)),
                dma((PIECES,)),
                dma((chips,)),
                dma((chips + SPLIT, PIECES + 1)),
                dma((1,)),
                dma((2, chips + SPLIT - 1, PIECES + 1)),
                dma((1,)),
                dma((2, chips - 1, PIECES)),
                dma((1,)),
                dma((1,)),
            ],
            compiler_params=pltpu.CompilerParams(
                collective_id=0, has_side_effects=True, vmem_limit_bytes=46 * 2**20
            ),
        )(x, dy, gate, up, w_gate, w_up, w_down)
        return pl.pallas_call(
            store,
            name="store",
            out_shape=[jax.ShapeDtypeStruct(s, BF16) for s in shapes],
            in_specs=[VMEM] * 4,
            out_specs=[ANY] * 4,
            scratch_shapes=[dma((4,))],
            compiler_params=pltpu.CompilerParams(vmem_limit_bytes=2**20),
        )(*(pltpu.with_memory_space_constraint(o, pltpu.VMEM) for o in outs))

    tokens, columns, down = P("dp", None), P(None, "tp"), P("tp", None)
    return jax.shard_map(
        step,
        mesh=mesh,
        in_specs=(tokens, tokens, P("dp", "tp"), P("dp", "tp"), columns, columns, down),
        out_specs=(tokens, P("dp", "tp"), P("dp", "tp"), P(("dp", "tp"), None)),
        check_vma=False,
    )
```

```python
import functools

import jax
import jax.numpy as jnp
from jax import lax
from jax.experimental import pallas as pl
from jax.experimental.pallas import tpu as pltpu
from jax.sharding import PartitionSpec as P

BF16, F32 = jnp.bfloat16, jnp.float32
ANY = pl.BlockSpec(memory_space=pl.ANY)
VMEM = pl.BlockSpec(memory_space=pltpu.VMEM)
PIECES = 4
SPLIT = 2
STORES = 16
TILE = 256


def dot(a, b, a_dim, b_dim):
    return lax.dot_general(a, b, (((a_dim,), (b_dim,)), ((), ())), preferred_element_type=F32)


def work(
    chips, x, dy, gate, up, w_gate, w_up, w_down, dx, wg, wu, wd,
    own, got, ring, mate, dys, dgu, hid, gs, us, wgu,
    load, wload, xload, pair_s, pair_r, rs_s, rs_r, ag_s, ag_r, fin_s, fin_r,
):
    rows, width = dx.shape
    hidden = wd.shape[0]
    block = rows // (4 * chips)
    part = width // PIECES
    t = lax.axis_index("tp")
    k, c = t // 2, t % 2
    around = [k] + [(k + i) % chips for i in range(1, chips)]
    right = {"tp": around[1] * 2 + c}
    left = {"tp": around[-1] * 2 + c}
    partner = {"tp": k * 2 + 1 - c}
    ways = (right, left)

    def origin(d, hops):
        return around[-hops] if d == 0 else around[hops]

    def row(chunk, d, core):
        return pl.multiple_of((chunk * 4 + d * 2 + core) * block, block)

    split = min(SPLIT, chips - 1)
    units = [(s, h) for s in range(split) for h in (0, 1)] + [(s, 0) for s in range(split, chips)]

    quarters, halves_of = [(q * part, part) for q in range(PIECES)], [(0, width // 2), (width // 2, width // 2)]
    pair_cuts = [[(0, part // 2), (part // 2, part // 2), *quarters[1:]]] + [quarters] * (len(units) - 1)
    sum_cuts = pair_cuts[: 2 * split] + [halves_of if s > 2 else quarters for s in range(split, chips)]
    last = [(0, 2 * part), (2 * part, part), (3 * part, part // 2), (3 * part + part // 2, part // 2)]
    gather_cuts = [halves_of] * (chips - 2) + [last]

    def within(cut, cuts):
        return [i for i, (a, n) in enumerate(cuts) if cut[0] <= a and a + n <= cut[0] + cut[1]]

    def high(s):
        return block // 2 if s < split else block

    def halves(s):
        return (0, 1) if s < split else (0,)

    def number(s, h):
        return units.index((s, h))

    def begin(s, h):
        return 4 * (s * block + h * high(s))

    def segments(s, h):
        todo = [around[-1 - s], around[(1 + s) % chips]]
        return [row(todo[d], d, core) + h * high(s) for core in (c, 1 - c) for d in (0, 1)]

    def load_dy(s, h):
        n = high(s)
        for i, r in enumerate(segments(s, h)):
            pltpu.make_async_copy(
                dy.at[pl.ds(r, n)], dys.at[pl.ds(begin(s, h) + i * n, n)], load.at[0, number(s, h)]
            ).start(priority=0 if (s, h) == (0, 0) else 1)

    def load_act(s, h):
        n = high(s)
        for i, r in enumerate(segments(s, h)):
            for m, (src, dst) in enumerate(((gate, gs), (up, us))):
                pltpu.make_async_copy(
                    src.at[pl.ds(r, n)],
                    dst.at[s % 2, pl.ds((h * 4 + i) * n, n)],
                    load.at[1 + m, number(s, h)],
                ).start(priority=0 if (s, h) == (0, 0) else 1)

    def load_x(b):
        for s, h in units:
            n = high(s)
            for i, r in enumerate(segments(s, h)):
                pltpu.make_async_copy(
                    x.at[pl.ds(r, n), pl.ds(b * part, part)],
                    wgu.at[pl.ds(begin(s, h) + i * n, n), pl.ds(b % 2 * part, part)],
                    xload.at[b],
                ).start(priority=1)

    def weights(q):
        band = pl.ds(q * part, part)
        return [
            pltpu.make_async_copy(src.at[band], wgu.at[band, pl.ds(m * hidden, hidden)], wload.at[m, q])
            for m, src in enumerate((w_gate, w_up))
        ]

    def start(copies):
        for copy in copies:
            copy.start(priority=1)

    def weights_down(i):
        n = TILE // PIECES
        for j in range(PIECES):
            band = pl.ds(i * TILE + j * n, n)
            pltpu.make_async_copy(w_down.at[band], wd.at[band], wload.at[2, i]).start()

    def wait_weights_down(i):
        band = pl.ds(i * TILE, TILE)
        pltpu.make_async_copy(w_down.at[band], wd.at[band], wload.at[2, i]).wait()

    load_act(0, 0)
    load_dy(0, 0)
    for i in range(hidden // TILE):
        weights_down(i)
    start(weights(0))

    barrier = pltpu.get_barrier_semaphore()
    for other in (right, left, partner):
        pl.semaphore_signal(barrier, inc=1, device_id=other)

    def remote(src, dst, send, recv, to):
        return pltpu.make_async_remote_copy(src_ref=src, dst_ref=dst, send_sem=send, recv_sem=recv, device_id=to)

    def sent(like, sem):
        pltpu.make_async_copy(like, like, sem).wait()

    def pair(s, h, i):
        u = number(s, h)
        at = (pl.ds(h * 2 * high(s), 2 * high(s)), pl.ds(*pair_cuts[u][i]))
        return remote(mate.at[s % 2, *at], got.at[s, *at], pair_s.at[s], pair_r.at[u, i], partner)

    def reduce(d, s, h, i):
        n, u = high(s), number(s, h)
        cols = pl.ds(*sum_cuts[u][i])
        return remote(
            got.at[s, pl.ds((h * 2 + d) * n, n), cols],
            ring.at[d, s, pl.ds(h * n, n), cols],
            rs_s.at[0],
            rs_r.at[d, u, i],
            ways[d],
        )

    def gather(d, hops, i):
        at = dx.at[pl.ds(row(origin(d, hops), d, c), block), pl.ds(*gather_cuts[hops][i])]
        return remote(at, at, ag_s.at[0], ag_r.at[d, hops, i], ways[d])

    def share(d, hops, cut):
        at = dx.at[pl.ds(row(origin(d, hops), d, c), block), pl.ds(*cut)]
        return remote(at, at, fin_s.at[0], fin_r.at[0], partner)

    def pass_on(s, h, i):
        n, u = high(s), number(s, h)
        cut = sum_cuts[u][i]
        cols = pl.ds(*cut)
        for j in within(cut, pair_cuts[u]):
            pair(s, h, j).wait_recv()
        for d in (0, 1):
            band = pl.ds((h * 2 + d) * n, n)
            total = own[s, band, cols] + got[s, band, cols].astype(F32)
            if s > 0:
                for before in (h,) if s < split else halves(s - 1):
                    for j in within(cut, sum_cuts[number(s - 1, before)]):
                        reduce(d, s - 1, before, j).wait_recv()
                total = total + ring[d, s - 1, pl.ds(h * n, n), cols].astype(F32)
            if s < chips - 1:
                got[s, band, cols] = total.astype(BF16)
            else:
                dx[pl.ds(row(k, d, c), block), cols] = total.astype(BF16)
        for d in (0, 1):
            if s < chips - 1:
                reduce(d, s, h, i).start()
            else:
                for j in within(cut, gather_cuts[0]):
                    gather(d, 0, j).start()
        if s == chips - 1:
            for d in (0, 1):
                share(d, 0, cut).start()

    def forward(hops, i):
        cut = gather_cuts[hops - 1][i]
        for d in (0, 1):
            gather(d, hops - 1, i).wait_recv()
            if hops < chips - 1:
                for j in within(cut, gather_cuts[hops]):
                    gather(d, hops, j).start()
            share(d, hops, cut).start()

    waiting = []

    def flush(lag=0):
        while waiting and begun[0] - waiting[0][1] >= lag:
            pass_on(*waiting.pop(0)[0])

    begun = [0]
    for s, h in units:
        n = high(s)
        here = pl.ds(begin(s, h), 4 * n)
        there = pl.ds(h * 4 * n, 4 * n)
        u = number(s, h)

        def gates(i, s=s, here=here, there=there):
            cols = pl.ds(pl.multiple_of(i * TILE, TILE), TILE)
            g = gs[s % 2, there, cols].astype(F32)
            v = us[s % 2, there, cols].astype(F32)
            sig = lax.logistic(g)
            silu = g * sig
            hid[here, cols] = (silu * v).astype(BF16)
            return silu, sig + g * (sig * (1.0 - sig)), v

        def back(i, silu, slope, v, here=here):
            cols = pl.ds(pl.multiple_of(i * TILE, TILE), TILE)
            up_cols = pl.ds(pl.multiple_of(hidden + i * TILE, TILE), TILE)
            dh = dot(dys[here], wd[cols, :], 1, 1)
            dgu[here, cols] = (dh * v * slope).astype(BF16)
            dgu[here, up_cols] = (dh * silu).astype(BF16)

        for m, (src, dst) in enumerate(((gate, gs), (up, us))):
            pltpu.make_async_copy(src.at[pl.ds(0, 4 * n)], dst.at[s % 2, there], load.at[1 + m, u]).wait()
        if s < split:
            for i in range(hidden // TILE):
                silu, slope, _ = gates(i)
                own[chips - 1, pl.ds(0, 4 * n), pl.ds(i * TILE, TILE)] = silu
                own[chips - 1, pl.ds(0, 4 * n), pl.ds(hidden + i * TILE, TILE)] = slope
            flush()
            pltpu.make_async_copy(dy.at[pl.ds(0, 4 * n)], dys.at[here], load.at[0, u]).wait()
            if u == 0:
                for i in range(hidden // TILE):
                    wait_weights_down(i)
                start(weights(1))
            silu = own[chips - 1, pl.ds(0, 4 * n), pl.ds(0, hidden)]
            slope = own[chips - 1, pl.ds(0, 4 * n), pl.ds(hidden, hidden)]
            dh = dot(dys[here], wd[...], 1, 1)
            dgu[here, pl.ds(0, hidden)] = (dh * us[s % 2, there, :].astype(F32) * slope).astype(BF16)
            dgu[here, pl.ds(hidden, hidden)] = (dh * silu).astype(BF16)
            if u == 0:
                for q in range(2, PIECES):
                    start(weights(q))
        else:
            pltpu.make_async_copy(dy.at[pl.ds(0, 4 * n)], dys.at[here], load.at[0, u]).wait()
            back(0, *gates(0))
            flush()
            for i in range(1, hidden // TILE):
                back(i, *gates(i))
        if u + 1 < len(units):
            load_dy(*units[u + 1])
            load_act(*units[u + 1])

        for i, cut in enumerate(pair_cuts[u]):
            if u == 0 and cut[0] % part == 0:
                for copy in weights(cut[0] // part):
                    copy.wait()
            if s >= 2 and h == 0 and i == 0:
                sent(got.at[0], pair_s.at[s - 2])
            cols = pl.ds(*cut)
            v = dot(dgu[here, :], wgu[cols, :], 1, 1)
            mate[s % 2, pl.ds(h * 2 * n, 2 * n), cols] = v[2 * n :].astype(BF16)
            if u == 0 and i == 0:
                pl.semaphore_wait(barrier, 3)
            pair(s, h, i).start()
            own[s, pl.ds(h * 2 * n, 2 * n), cols] = v[: 2 * n]
            begun[0] += 1
            for j, whole in enumerate(sum_cuts[u]):
                if within(whole, pair_cuts[u])[-1] == i:
                    waiting.append(((s, h, j), begun[0]))
            flush(2 if s < split else 1)
        if (s, h) == units[-1]:
            load_x(0)
            load_x(1)
    flush()

    events = [(hops, i) for hops in range(1, chips) for i in range(len(gather_cuts[hops - 1]))]

    for b in range(PIECES):
        band = pl.ds(b * part, part)
        slot = pl.ds(b % 2 * part, part)

        @pl.loop(0, part // TILE)
        def _(i, b=b):
            cols = pl.ds(pl.multiple_of(b * part + i * TILE, TILE), TILE)
            wd[:, cols] = dot(hid[...], dys[:, cols], 0, 0).astype(BF16)

        if b == PIECES - 1:
            forward(*events.pop(0))
        pltpu.make_async_copy(x.at[:, band], wgu.at[:, slot], xload.at[b]).wait()

        for m, out in enumerate((wg, wu)):

            @pl.loop(0, hidden // TILE)
            def _(i, m=m, out=out, band=band, slot=slot):
                cols = pl.ds(pl.multiple_of(i * TILE, TILE), TILE)
                from_cols = pl.ds(pl.multiple_of(m * hidden + i * TILE, TILE), TILE)
                out[band, cols] = dot(wgu[:, slot], dgu[:, from_cols], 0, 0).astype(BF16)

            if (b, m) in ((0, 1), (1, 0), (2, 0)):
                forward(*events.pop(0))
        if b + 2 < PIECES:
            load_x(b + 2)

    while events:
        forward(*events.pop(0))

    for s in range(max(chips - 2, 0), chips):
        sent(got.at[0], pair_s.at[s])
    sent(dx.at[pl.ds(0, 2 * (chips - 1) * block)], rs_s.at[0])
    sent(dx.at[pl.ds(0, 2 * (chips - 1) * block)], ag_s.at[0])
    sent(dx.at[pl.ds(0, 2 * chips * block)], fin_s.at[0])
    sent(dx.at[pl.ds(0, 2 * chips * block)], fin_r.at[0])


def store(*refs):
    n = (len(refs) - 1) // 2
    sems = refs[-1]
    for i, (src, dst) in enumerate(zip(refs[:n], refs[n:-1])):
        size = src.shape[0] // STORES
        for p in range(STORES):
            at = pl.ds(p * size, size)
            pltpu.make_async_copy(src.at[at], dst.at[at], sems.at[i]).start()
    for i, (src, dst) in enumerate(zip(refs[:n], refs[n:-1])):
        pltpu.make_async_copy(src, dst, sems.at[i]).wait()


def solution(mesh):
    chips = mesh.shape["tp"] // 2

    def step(x, dy, gate, up, w_gate, w_up, w_down):
        rows, width = x.shape
        hidden = gate.shape[1]
        block = rows // (4 * chips)
        shapes = ((rows, width), w_gate.shape, w_up.shape, w_down.shape)
        dma = pltpu.SemaphoreType.DMA
        outs = pl.pallas_call(
            functools.partial(work, chips),
            name="work",
            out_shape=[pltpu.VMEM(s, BF16) for s in shapes],
            in_specs=[ANY] * 7,
            out_specs=[VMEM] * 4,
            scratch_shapes=[
                pltpu.VMEM((chips, 2 * block, width), F32),
                pltpu.VMEM((chips, 2 * block, width), BF16),
                pltpu.VMEM((2, chips - 1, block, width), BF16),
                pltpu.VMEM((2, 2 * block, width), BF16),
                pltpu.VMEM((rows, width), BF16),
                pltpu.VMEM((rows, 2 * hidden), BF16),
                pltpu.VMEM((rows, hidden), BF16),
                pltpu.VMEM((2, 4 * block, hidden), BF16),
                pltpu.VMEM((2, 4 * block, hidden), BF16),
                pltpu.VMEM((width, 2 * hidden), BF16),
                dma((3, chips + SPLIT)),
                dma((3, PIECES)),
                dma((PIECES,)),
                dma((chips,)),
                dma((chips + SPLIT, PIECES + 1)),
                dma((1,)),
                dma((2, chips + SPLIT - 1, PIECES + 1)),
                dma((1,)),
                dma((2, chips - 1, PIECES)),
                dma((1,)),
                dma((1,)),
            ],
            compiler_params=pltpu.CompilerParams(
                collective_id=0, has_side_effects=True, vmem_limit_bytes=46 * 2**20
            ),
        )(x, dy, gate, up, w_gate, w_up, w_down)
        return pl.pallas_call(
            store,
            name="store",
            out_shape=[jax.ShapeDtypeStruct(s, BF16) for s in shapes],
            in_specs=[VMEM] * 4,
            out_specs=[ANY] * 4,
            scratch_shapes=[dma((4,))],
            compiler_params=pltpu.CompilerParams(vmem_limit_bytes=2**20),
        )(*(pltpu.with_memory_space_constraint(o, pltpu.VMEM) for o in outs))

    tokens, columns, down = P("dp", None), P(None, "tp"), P("tp", None)
    return jax.shard_map(
        step,
        mesh=mesh,
        in_specs=(tokens, tokens, P("dp", "tp"), P("dp", "tp"), columns, columns, down),
        out_specs=(tokens, P("dp", "tp"), P("dp", "tp"), P(("dp", "tp"), None)),
        check_vma=False,
    )
```
